32 devices in a mesh: tm: 8 (over y, x, core), chan: 4 (over z).
Axes of the slice: x: 2, y: 2, z: 4, core: 2. Of those that a mesh axis runs over, the one named last changes fastest.
Arguments:
- auxiliary: float32 [512, 262144], P('chan', 'tm'), may hold values from -30 to 30
- proofs: float32 [64, 262144], P('chan', 'tm'), may hold values from -12 to 12
Outputs:
- coherence: float32 [512, 64, 4096], P('chan', None, 'tm')
The draws below stay inside these ranges and needn't reach their ends.
All inputs are finite; a program needn't handle non-finite values.
Results may differ from the reference program's by a relative error of at most 0.00076.
Values may be sent and summed in bfloat16 or wider, within the bound.
A program may use at most 192 MiB of HBM per device.

```python
import math
import jax
import jax.numpy as jnp
from jax import lax

AUX_CH = 512
WIT_CH = 64
SEG_LEN = 8192
STRIDE = 4096
BINS = 4096
SEGMENTS = 63
SAMPLES = 262144


def coupled_series(key):
    subkeys = [jax.random.fold_in(key, 101 + number) for number in range(9)]
    moments = jnp.arange(SAMPLES, dtype=jnp.float32) / SAMPLES
    wit_noise = jax.random.truncated_normal(subkeys[0], -6.0, 6.0, (WIT_CH, SAMPLES), jnp.float32)
    aux_noise = jax.random.truncated_normal(subkeys[1], -6.0, 6.0, (AUX_CH, SAMPLES), jnp.float32)
    spread = 1.0
    wit_offset = jax.random.uniform(subkeys[2], (WIT_CH,), jnp.float32, -spread, spread)
    proof_out = wit_noise + wit_offset[:, None] * (0.5 + moments)[None, :]
    target = jax.random.randint(subkeys[3], (AUX_CH,), 0, WIT_CH)
    delays = jax.random.randint(subkeys[4], (AUX_CH,), 0, 4)
    gains_aux = jax.random.uniform(subkeys[5], (AUX_CH,), jnp.float32, 0.0, 2.0)
    source = wit_noise[target]
    shifted = jax.vmap(lambda series_row, amount: jnp.roll(series_row, amount))(source, delays)
    aux_offset = jax.random.uniform(subkeys[6], (AUX_CH,), jnp.float32, -spread, spread)
    aux_out = aux_noise + gains_aux[:, None] * shifted + aux_offset[:, None] * (1.0 + 2.0 * moments)[None, :]
    return (aux_out, proof_out)


def draw_auxiliary(key, part):
    return coupled_series(key)[0]


def draw_proofs(key, part):
    return coupled_series(key)[1]


def setup_inputs(seed: int = 0) -> dict:
    seeds = jax.random.split(jax.random.key(seed), 3)
    auxiliary = draw_auxiliary(jax.random.fold_in(seeds[2], 71), 0)
    proofs = draw_proofs(jax.random.fold_in(seeds[2], 71), 0)
    return dict(auxiliary=auxiliary, proofs=proofs)


def spectra_of(series, channel_means):
    row_count = series.shape[0]
    blocks = series.reshape(row_count, SEGMENTS + 1, STRIDE)
    segments = jnp.concatenate([blocks[:, :-1], blocks[:, 1:]], axis=2)
    position = jnp.arange(SEG_LEN, dtype=jnp.float32)
    window = 0.5 - 0.5 * jnp.cos(2.0 * math.pi * position / SEG_LEN)
    windowed = (segments - channel_means[:, None, None]) * window
    spectrum = jnp.fft.rfft(windowed, axis=-1)[..., :BINS]
    return jnp.real(spectrum).astype(jnp.bfloat16), jnp.imag(spectrum).astype(jnp.bfloat16)


def reference(auxiliary, proofs):
    aux_means = jnp.sum(auxiliary, axis=1) / SAMPLES
    wit_means = jnp.sum(proofs, axis=1) / SAMPLES
    wit_real, wit_imag = spectra_of(proofs, wit_means)
    wit_real = wit_real.astype(jnp.float32)
    wit_imag = wit_imag.astype(jnp.float32)
    wit_power = jnp.sum(wit_real * wit_real + wit_imag * wit_imag, axis=1)
    block_size = math.gcd(AUX_CH, 8)
    aux_blocks = auxiliary.reshape(AUX_CH // block_size, block_size, SAMPLES)
    mean_blocks = aux_means.reshape(AUX_CH // block_size, block_size)

    def one_block(block_pair):
        rows_here, block_means = block_pair
        aux_real, aux_imag = spectra_of(rows_here, block_means)
        aux_real = aux_real.astype(jnp.float32)
        aux_imag = aux_imag.astype(jnp.float32)
        cross_real = jnp.einsum("csf,wsf->cwf", aux_real, wit_real) + jnp.einsum("csf,wsf->cwf", aux_imag, wit_imag)
        cross_imag = jnp.einsum("csf,wsf->cwf", aux_imag, wit_real) - jnp.einsum("csf,wsf->cwf", aux_real, wit_imag)
        aux_power = jnp.sum(aux_real * aux_real + aux_imag * aux_imag, axis=1)
        return (cross_real * cross_real + cross_imag * cross_imag) / ((aux_power[:, None, :] + 1e-6) * (wit_power[None, :, :] + 1e-6))

    result = lax.map(one_block, (aux_blocks, mean_blocks))
    return result.reshape(AUX_CH, WIT_CH, BINS)
```

```python
import functools
import math

import jax
import jax.numpy as jnp
import numpy as np
from jax import lax
from jax.experimental import pallas as pl
from jax.experimental.pallas import tpu as pltpu
from jax.sharding import PartitionSpec as P

SEG_LEN = 8192
STRIDE = 4096
BINS = 4096
LANES = 128
ROWS = SEG_LEN // LANES
HALF = STRIDE // LANES
INNER = SEG_LEN // LANES
MS = BINS // LANES


def split_high_low(value):
    high = value.astype(jnp.bfloat16)
    low = (value - high.astype(jnp.float32)).astype(jnp.bfloat16)
    return high, low


def tables():
    position = np.arange(SEG_LEN, dtype=np.float64)
    window = (0.5 - 0.5 * np.cos(2.0 * np.pi * position / SEG_LEN)).reshape(ROWS, LANES)
    k1 = np.arange(LANES)
    first = np.zeros((2, 2, ROWS, 2, 2, LANES))
    for half in range(2):
        p = 2 * np.arange(ROWS) + half
        angle = 2.0 * np.pi * (np.outer(p, k1) % LANES) / LANES
        for pair in range(2):
            first[half, pair, :, pair, 0] = np.cos(angle)
            first[half, pair, :, pair, 1] = -np.sin(angle)
    first = first.reshape(4 * ROWS, 4 * LANES)
    q = np.arange(INNER)
    twist = 2.0 * np.pi * np.outer(q, k1) / SEG_LEN
    m = np.arange(MS)
    angle = 2.0 * np.pi * (np.outer(m, q) % INNER) / INNER
    cos, sin = np.cos(angle), np.sin(angle)
    second = np.block([[cos, sin], [-sin, cos]])
    first = jnp.asarray(first, jnp.float32)
    second = jnp.asarray(second, jnp.float32)
    first_high, first_low = split_high_low(first)
    second_high, second_low = split_high_low(second)
    stacked = jnp.concatenate(
        [
            jnp.concatenate([second_high, second_high], axis=1),
            jnp.concatenate([second_low, jnp.zeros_like(second_low)], axis=1),
        ],
        axis=0,
    )
    return (
        jnp.asarray(window, jnp.float32),
        first_high,
        first_low,
        jnp.asarray(np.cos(twist), jnp.float32),
        jnp.asarray(np.sin(twist), jnp.float32),
        stacked,
    )


def transform_kernel(
    seg_count, dests, x_ref, halo_ref, corr_ref, keep_ref, window_ref, fh_ref, fl_ref,
    cos_ref, sin_ref, g_ref, out_ref
):
    per = MS // dests

    def one_channel(c, carry):
        window = window_ref[...]
        cos, sin = cos_ref[...], sin_ref[...]
        blocks = [x_ref[c, pl.ds(HALF * s, HALF), :] for s in range(seg_count)]
        blocks.append(halo_ref[c])
        lefts = []
        for pair in range(seg_count // 2):
            s = 2 * pair
            stacked = jnp.concatenate(
                [
                    jnp.concatenate([blocks[s], blocks[s + 1]], axis=0) * window,
                    jnp.concatenate([blocks[s + 1], blocks[s + 2]], axis=0) * window,
                ],
                axis=0,
            )
            turned = stacked.T
            lefts.append(jnp.concatenate([turned[:INNER], turned[INNER:]], axis=1))
        left = jnp.concatenate(lefts, axis=0)
        high, low = split_high_low(left)
        fh = fh_ref[...]
        y = (
            jnp.dot(high, fh, preferred_element_type=jnp.float32)
            + jnp.dot(low, fh, preferred_element_type=jnp.float32)
            + jnp.dot(high, fl_ref[...], preferred_element_type=jnp.float32)
        )
        for pair in range(seg_count // 2):
            yy = y[INNER * pair : INNER * (pair + 1)]
            columns = []
            for j in range(2):
                re = yy[:, (2 * j) * LANES : (2 * j + 1) * LANES]
                im = yy[:, (2 * j + 1) * LANES : (2 * j + 2) * LANES]
                turned = jnp.concatenate([re * cos + im * sin, im * cos - re * sin], axis=0)
                columns.append(turned)
            both = jnp.concatenate(columns, axis=1)
            bh, bl = split_high_low(both)
            z = jnp.dot(
                g_ref[...], jnp.concatenate([bh, bl], axis=0), preferred_element_type=jnp.float32
            )
            z = z[: 2 * MS] + z[2 * MS :]
            for j in range(2):
                s = 2 * pair + j
                keep = keep_ref[pl.ds(s, 1), :]
                zs = z[:, j * LANES : (j + 1) * LANES]
                real = jnp.concatenate([zs[:8] + corr_ref[c], zs[8:MS]], axis=0)
                real = (real * keep).astype(jnp.bfloat16)
                imag = (zs[MS:] * keep).astype(jnp.bfloat16)
                for d in range(dests):
                    out_ref[d, 0, c, s] = real[per * d : per * (d + 1)]
                    out_ref[d, 1, c, s] = imag[per * d : per * (d + 1)]
        return carry

    lax.fori_loop(0, x_ref.shape[0], one_channel, 0)


def transform(series, halo, corr, keep, tabs, dests):
    channels = series.shape[0]
    seg_count = series.shape[1] // HALF
    block = math.gcd(channels, 8)
    per = MS // dests
    whole = lambda a: pl.BlockSpec(a.shape, lambda i: (0,) * a.ndim)
    return pl.pallas_call(
        functools.partial(transform_kernel, seg_count, dests),
        grid=(channels // block,),
        in_specs=[
            pl.BlockSpec((block,) + series.shape[1:], lambda i: (i, 0, 0)),
            pl.BlockSpec((block,) + halo.shape[1:], lambda i: (i, 0, 0)),
            pl.BlockSpec((block,) + corr.shape[1:], lambda i: (i, 0, 0)),
            whole(keep),
        ]
        + [whole(a) for a in tabs],
        out_specs=pl.BlockSpec(
            (dests, 2, block, seg_count, per, LANES), lambda i: (0, 0, i, 0, 0, 0)
        ),
        out_shape=jax.ShapeDtypeStruct(
            (dests, 2, channels, seg_count, per, LANES), jnp.bfloat16
        ),
        compiler_params=pltpu.CompilerParams(
            dimension_semantics=("arbitrary",), vmem_limit_bytes=48 * 1024 * 1024
        ),
    )(series, halo, corr, keep, *tabs)


def shifted(value, axis, by):
    peers = lax.axis_size(axis)
    pairs = [(i, i + by) for i in range(peers) if 0 <= i + by < peers]
    return lax.ppermute(value, axis, pairs)


def gather_channels(piece, axis):
    peers = lax.axis_size(axis)
    me = lax.axis_index(axis)
    rows = piece.shape[1]
    whole = jnp.zeros((piece.shape[0], rows * peers) + piece.shape[2:], piece.dtype)
    whole = lax.dynamic_update_slice_in_dim(whole, piece, me * rows, 1)
    for step in range(1, peers):
        moved = lax.ppermute(piece, axis, [(i, (i + step) % peers) for i in range(peers)])
        owner = lax.rem(me - step + peers, peers)
        whole = lax.dynamic_update_slice_in_dim(whole, moved, owner * rows, 1)
    return whole


def exchange(spectra):
    moved = lax.all_to_all(spectra, "tm", split_axis=0, concat_axis=0, tiled=True)
    moved = moved.transpose(1, 2, 0, 3, 4, 5)
    parts, channels, sources, segs, per, lanes = moved.shape
    return moved.reshape(parts, channels, sources * segs, per * lanes)


def per_device(auxiliary, proofs):
    aux_rows = auxiliary.shape[0]
    wit_rows = proofs.shape[0]
    tm_size = lax.axis_size("tm")
    seg_count = auxiliary.shape[1] // STRIDE
    tabs = tables()
    wit_series = proofs.reshape(wit_rows, -1, LANES)
    aux_series = auxiliary.reshape(aux_rows, -1, LANES)
    next_wit = shifted(proofs[:, :STRIDE], "tm", -1).reshape(wit_rows, HALF, LANES)
    next_aux = shifted(auxiliary[:, :STRIDE], "tm", -1).reshape(aux_rows, HALF, LANES)
    sums = jnp.concatenate([jnp.sum(proofs, axis=1), jnp.sum(auxiliary, axis=1)])
    totals = jnp.sum(lax.all_gather(sums, "tm"), axis=0)
    means = totals / (auxiliary.shape[1] * tm_size)
    place = np.zeros((8, LANES), np.float32)
    place[0, 0] = -0.5 * SEG_LEN
    place[0, 1] = 0.25 * SEG_LEN
    corr = means[:, None, None] * place[None]
    last = lax.axis_index("tm") == tm_size - 1
    seg_index = jnp.arange(seg_count)[:, None] + jnp.zeros((1, LANES), jnp.int32)
    keep = jnp.where(last & (seg_index == seg_count - 1), 0.0, 1.0).astype(jnp.float32)
    wit_spec = transform(wit_series, next_wit, corr[:wit_rows], keep, tabs, tm_size)
    wit = gather_channels(exchange(wit_spec), "chan")
    aux_spec = transform(aux_series, next_aux, corr[wit_rows:], keep, tabs, tm_size)
    aux = exchange(aux_spec)
    aux_float = aux.astype(jnp.float32)
    aux_power = jnp.sum(aux_float * aux_float, axis=(0, 2))
    wit_float = wit.astype(jnp.float32)
    wit_power = jnp.sum(wit_float * wit_float, axis=(0, 2))
    left_real = jnp.concatenate([aux[0], aux[1]], axis=1)
    left_imag = jnp.concatenate([aux[1], -aux[0]], axis=1)
    right_side = jnp.concatenate([wit[0], wit[1]], axis=1)
    cross_real = jnp.einsum(
        "csf,wsf->cwf", left_real, right_side, preferred_element_type=jnp.float32
    )
    cross_imag = jnp.einsum(
        "csf,wsf->cwf", left_imag, right_side, preferred_element_type=jnp.float32
    )
    return (cross_real * cross_real + cross_imag * cross_imag) / (
        (aux_power[:, None, :] + 1e-06) * (wit_power[None, :, :] + 1e-06)
    )


def solution(mesh):
    return jax.shard_map(
        per_device,
        mesh=mesh,
        in_specs=(P("chan", "tm"), P("chan", "tm")),
        out_specs=P("chan", None, "tm"),
        check_vma=False,
    )
```
